32 devices in a mesh: node: 32 (over z, y, x, core).
Axes of the slice: x: 2, y: 2, z: 4, core: 2. Of those that a mesh axis runs over, the one named last changes fastest.
Arguments:
- labels: bfloat16 [131072, 512], P('node'), may hold values from -6 to 6
- seed_mask: int32 [131072], P('node'), may hold values 0 or 1
- band_w: bfloat16 [1024, 3, 128, 128], P('node'), may hold values from 0.0009994507 to 1
- far_block: int32 [32, 32, 2], P('node'), may hold values from 0 to 511
- far_tile: int32 [32, 32, 2], P('node'), may hold values from 0 to 31
- far_count: int32 [32, 32], P('node'), may hold values from 0 to 2, as said below
- far_w: bfloat16 [32, 32, 2, 8, 128], P('node'), may hold values from 0.049804688 to 2
Outputs:
- final_labels: bfloat16 [131072, 512], P('node')
- residual: float32 [2, 1024], P(None, 'node')
The draws below stay inside these ranges and needn't reach their ends.
Inputs may be any that keep to these rules, and one draw needn't show every extreme that they name: `far_count`: in every draw at least one destination shard has all 2 slots live from every source shard; other counts vary from pair to pair.
All inputs are finite; a program needn't handle non-finite values. No bound on the sum of `seed_mask` on one device may be relied on, other than what follows from the above.
Results may differ from the reference program's by a relative error of at most 0.0027.
Values may be sent and summed in bfloat16 or wider, within the bound.
A program may use at most 128 MiB of HBM per device.

```python
import math
import jax
import jax.numpy as jnp
from jax import lax

C = 512
NODE_DEV = 4096
TILE = 128
BLK = 8
SLOTS = 2
ITERS = 2
NODES = 131072
N_NODE = 32


def draw_far_count(key, part):
    first_key, second_key = jax.random.split(jax.random.fold_in(key, 17))
    counts = jax.random.randint(first_key, (N_NODE, N_NODE), 0, SLOTS + 1)
    busiest = jax.random.randint(second_key, (), 0, N_NODE)
    row_ids = jnp.arange(N_NODE)[:, None]
    return jnp.where(row_ids == busiest, SLOTS, counts).astype(jnp.int32)


def set_ends(values, rng, smallest, top_value):
    dims = values.shape
    place = [jax.random.randint(jax.random.fold_in(rng, axis), (), 0, dims[axis]) for axis in range(len(dims))]
    values = values.at[tuple(place)].set(smallest)
    longest = dims.index(max(dims))
    place[longest] = (place[longest] + 1) % dims[longest]
    return values.at[tuple(place)].set(top_value)


def block_scale(own_key, dims, cuts, smallest, high):
    factor_of, own = 1.0, jax.random.fold_in(own_key, 6)
    for dim, parts in cuts:
        steps = jnp.exp(jax.random.uniform(jax.random.fold_in(own, dim), (parts,), jnp.float32, smallest / len(cuts), high / len(cuts)))
        factor_of = factor_of * jnp.repeat(steps, dims[dim] // parts).reshape([-1 if axis == dim else 1 for axis in range(len(dims))])
    return factor_of


def normal_values(own_key, shape, width, most, pieces=(), dtype=jnp.bfloat16):
    array = width * jax.random.normal(own_key, shape, jnp.float32)
    if pieces:
        array = array * block_scale(own_key, shape, pieces, -0.22, 0.18)
    return jnp.clip(array, -most, most).astype(dtype)


def setup_inputs(seed: int = 0) -> dict:
    key_of = jax.random.split(jax.random.key(seed), 8)
    return {
        "labels": normal_values(key_of[0], (NODES, C), 1.0, 6.0, ((0, 32),)),
        "seed_mask": set_ends((jax.random.randint(key_of[1], (NODES,), 0, 4) < 1).astype(jnp.int32), jax.random.fold_in(key_of[1], 1), 0, 1),
        "band_w": jnp.clip(jnp.exp(math.log(1.0) - 6.9083047 * jax.random.uniform(key_of[2], (NODES // TILE, 3, TILE, TILE), jnp.float32) ** block_scale(key_of[2], (NODES // TILE, 3, TILE, TILE), ((0, 32),), -0.2, 0.2)), 0.0009994507, 1.0).astype(jnp.bfloat16),
        "far_block": set_ends(jax.random.randint(key_of[3], (N_NODE, N_NODE, SLOTS), 0, NODE_DEV // BLK), jax.random.fold_in(key_of[3], 1), 0, (NODE_DEV // BLK) - 1).astype(jnp.int32),
        "far_tile": set_ends(jax.random.randint(key_of[4], (N_NODE, N_NODE, SLOTS), 0, NODE_DEV // TILE), jax.random.fold_in(key_of[4], 1), 0, (NODE_DEV // TILE) - 1).astype(jnp.int32),
        "far_count": draw_far_count(jax.random.fold_in(key_of[7], 71), 0),
        "far_w": jnp.clip(jnp.exp(math.log(2.0) - 3.6927934 * jax.random.uniform(key_of[6], (N_NODE, N_NODE, SLOTS, BLK, TILE), jnp.float32) ** block_scale(key_of[6], (N_NODE, N_NODE, SLOTS, BLK, TILE), ((0, 32),), -0.2, 0.2)), 0.049804688, 2.0).astype(jnp.bfloat16),
    }


def live_table(count_row):
    return (jnp.arange(SLOTS)[None, :] < count_row[:, None]).astype(jnp.float32)

def reference(labels, seed_mask, band_w, far_block, far_tile, far_count, far_w):
    tile_total = labels.shape[0] // TILE
    block_count = NODE_DEV // BLK
    band_wide = band_w.astype(jnp.float32)
    degree_band = lax.optimization_barrier(jnp.sum(band_wide, axis=(1, 3)))

    def far_degree(packed):
        tiles_here, count_here, weight_here = packed
        live_weights = weight_here.astype(jnp.float32) * live_table(count_here)[:, :, None, None]
        weight_sums = lax.optimization_barrier(jnp.sum(live_weights, axis=2)).reshape(-1, TILE)
        return jnp.zeros((NODE_DEV // TILE, TILE), jnp.float32).at[tiles_here.reshape(-1)].add(weight_sums)
    degree_far = lax.map(far_degree, (far_tile, far_count, far_w)).reshape(tile_total, TILE)
    degree = degree_band + degree_far
    seeded = (seed_mask == 1).reshape(tile_total, TILE, 1)
    clamped = labels.astype(jnp.float32).reshape(tile_total, TILE, C)
    current = labels
    residuals = []
    for sweep in range(ITERS):
        tiles = current.astype(jnp.float32).reshape(tile_total, TILE, C)
        band_sum = jnp.zeros((tile_total, TILE, C), jnp.float32)
        for offset in (-1, 0, 1):
            source = jnp.roll(tiles, -offset, axis=0)
            band_sum = band_sum + jnp.einsum('itr,irc->itc', band_wide[:, offset + 1], source)
        blocks_all = current.reshape(N_NODE, block_count, BLK, C)

        def far_part(packed):
            wanted, tiles_here, count_here, weight_here = packed
            blocks = blocks_all[jnp.arange(N_NODE)[:, None], wanted].astype(jnp.float32)
            live_weights = weight_here.astype(jnp.float32) * live_table(count_here)[:, :, None, None]
            contrib = jnp.einsum('skqt,skqc->sktc', live_weights, blocks)
            return jnp.zeros((NODE_DEV // TILE, TILE, C), jnp.float32).at[tiles_here.reshape(-1)].add(contrib.reshape(-1, TILE, C))
        far_sum = lax.map(far_part, (far_block, far_tile, far_count, far_w)).reshape(tile_total, TILE, C)
        averaged = (band_sum + far_sum) / degree[:, :, None]
        row_scale = jnp.sqrt(lax.optimization_barrier(jnp.mean(averaged * averaged, axis=2, keepdims=True)))
        scaled = averaged / jnp.maximum(row_scale, 0.05)
        fresh = jnp.where(seeded, clamped, scaled).astype(jnp.bfloat16)
        residuals.append(lax.optimization_barrier(jnp.sum(jnp.abs(fresh.astype(jnp.float32) - tiles), axis=(1, 2))))
        current = fresh.reshape(labels.shape[0], C)
    return (current, jnp.stack(residuals))
```

```python
import functools

import jax
import jax.numpy as jnp
from jax import lax
from jax.experimental import pallas as pl
from jax.experimental.pallas import tpu as pltpu
from jax.sharding import PartitionSpec as P

ITERS = 2
CHUNKS = 2
MESH = pl.DeviceIdType.MESH
ROWS = 32
GROUP = 16
SUB = 8
LANE = 128
WIDE = 256
FLOOR = 0.05
BAND_UNROLL = 7
FAR_UNROLL = 4
SEND_UNROLL = 4
SCALE_UNROLL = 16
PREP_UNROLL = 4


def kernel(
    dims,
    labels_hbm, band_hbm, farw_hbm, req_ref, tile_ref, count_ref, seed_ref,
    out_ref, res_ref,
    cur0, cur1, band, farw, wide_t, onehot, placed, acc, far_a, far_b, limit, kept, fac, part,
    halo0, halo1, send, recv, fac_out, fac_in, req_s,
    lab_sem, band_sem, farw_sem, smem_sem,
    req_send, req_recv, halo_send, halo_recv, blk_send, blk_recv, fac_send, fac_recv,
):
    n, tiles, tile, slots, blk, classes = dims
    rows = tiles * tile
    per = slots * blk
    far_rows = n * per
    width = classes // CHUNKS
    me = lax.axis_index("node")
    right, left = lax.rem(me + 1, n), lax.rem(me + n - 1, n)
    cur = (cur0, cur1)
    halo = (halo0, halo1)
    others = pl.ds(0, n - 1)
    pairs = tiles // 2

    def columns(c):
        return slice(c * width, (c + 1) * width)

    def groups(start, size):
        return pl.ds(start // GROUP, size // GROUP)

    def as_rows(value):
        return value.reshape(-1, value.shape[-1])

    barrier = pltpu.get_barrier_semaphore()

    @pl.loop(1, n)
    def _(j):
        pl.semaphore_signal(barrier, inc=1, device_id=(lax.rem(me + j, n),), device_id_type=MESH)

    lab_copy = pltpu.make_async_copy(labels_hbm, cur0.at[groups(tile, rows)], lab_sem)
    band_copy = pltpu.make_async_copy(band_hbm, band, band_sem)
    farw_copy = pltpu.make_async_copy(farw_hbm, farw, farw_sem)
    own_req = pltpu.make_async_copy(req_ref, req_s.at[me], smem_sem)
    own_req.start()
    farw_copy.start()
    band_copy.start()
    lab_copy.start()

    pl.semaphore_wait(barrier, n - 1)

    @pl.loop(1, n)
    def _(j):
        peer = lax.rem(me + j, n)
        pltpu.make_async_remote_copy(
            req_ref, req_s.at[me], req_send, req_recv,
            device_id=(peer,), device_id_type=MESH,
        ).start()

    def halo_copies(it, low, high):
        return (
            pltpu.make_async_remote_copy(
                high, halo[it].at[0], halo_send.at[it, 0], halo_recv.at[it, 0],
                device_id=(right,), device_id_type=MESH,
            ),
            pltpu.make_async_remote_copy(
                low, halo[it].at[1], halo_send.at[it, 1], halo_recv.at[it, 1],
                device_id=(left,), device_id_type=MESH,
            ),
        )

    halo_first = halo_copies(
        0, labels_hbm.at[groups(0, tile)], labels_hbm.at[groups(rows - tile, tile)]
    )
    for copy in halo_first:
        copy.start()

    def block_copy(it, c, j):
        peer = lax.rem(me + j, n)
        return pltpu.make_async_remote_copy(
            send.at[it, c, peer], recv.at[it, c, me], blk_send.at[it, c], blk_recv.at[it, c],
            device_id=(peer,), device_id_type=MESH,
        )

    def factor_copy(j):
        peer = lax.rem(me + j, n)
        return pltpu.make_async_remote_copy(
            fac_out.at[peer], fac_in.at[me], fac_send, fac_recv,
            device_id=(peer,), device_id_type=MESH,
        )

    def block_of(it, c, wanted):
        pair = cur[it][wanted // 2 + tile // GROUP, :, columns(c)].astype(jnp.float32)
        odd = jnp.full((blk, width), wanted % 2, jnp.int32) == 1
        return jnp.where(odd, pair[blk:], pair[:blk])

    def gathered(it, c, peer, raw):
        halves = []
        for k in range(slots):
            wanted = req_s[peer, k, me]
            if raw:
                seeded = jnp.concatenate([limit[wanted]] * (width // LANE), axis=1) < 0.0
                halves.append(
                    jnp.where(seeded, block_of(0, c, wanted), acc[wanted, :, columns(c)])
                )
            else:
                halves.append(block_of(it, c, wanted))
        return jnp.concatenate(halves, axis=0).astype(jnp.bfloat16)

    def send_all(fill, copy):
        @pl.loop(0, n // SEND_UNROLL)
        def _(q):
            for u in range(SEND_UNROLL):
                fill(lax.rem(me + q * SEND_UNROLL + u + 1, n))

            @pl.when(q > 0)
            def _():
                for u in range(SEND_UNROLL):
                    copy((q - 1) * SEND_UNROLL + u + 1).start()

    def send_rest(copy):
        for j in range(n - SEND_UNROLL + 1, n):
            copy(j).start()

    def exchange(it, c, raw=False):
        def fill(peer):
            send[it, c, peer] = gathered(it, c, peer, raw)

        def copy(j):
            return block_copy(it, c, j)

        send_all(fill, copy)
        recv[it, c, me] = send[it, c, me]
        send_rest(copy)

    diagonal = lax.broadcasted_iota(jnp.int32, (per, LANE), 0) == lax.broadcasted_iota(
        jnp.int32, (per, LANE), 1
    )

    def factors_for(peer):
        both = jnp.concatenate([fac[req_s[peer, k, me]] for k in range(slots)], axis=0)
        return jnp.sum(jnp.where(diagonal, both, 0.0), axis=0, keepdims=True)

    def exchange_factors():
        def fill(peer):
            fac_out[peer] = factors_for(peer)

        send_all(fill, factor_copy)
        fac_in[me] = fac_out[me]
        send_rest(factor_copy)

    def await_factors():
        pltpu.make_async_copy(fac_out.at[others], fac_out.at[others], fac_send).wait()
        pltpu.make_async_copy(fac_in.at[others], fac_in.at[others], fac_recv).wait()

    def await_halo(it, copies):
        for copy in copies:
            copy.wait()
        cur[it][groups(0, tile)] = halo[it][0]
        cur[it][groups(rows + tile, tile)] = halo[it][1]

    def await_blocks(it, c):
        out_going, coming = send.at[it, c, others], recv.at[it, c, others]
        pltpu.make_async_copy(out_going, out_going, blk_send.at[it, c]).wait()
        pltpu.make_async_copy(coming, coming, blk_recv.at[it, c]).wait()

    def scale_received(it, c):
        @pl.loop(0, n // SCALE_UNROLL)
        def _(q):
            for u in range(SCALE_UNROLL):
                s = q * SCALE_UNROLL + u
                column = jnp.sum(
                    jnp.where(diagonal, jnp.broadcast_to(fac_in[s], (per, LANE)), 0.0),
                    axis=1, keepdims=True,
                )
                value = recv[it, c, s].astype(jnp.float32) * column
                recv[it, c, s] = value.astype(jnp.bfloat16)

    def band_pairs(it, first, count):
        zero = jnp.zeros((tile, tile), jnp.bfloat16)
        for u in range(count):
            p = first + u
            upper = [band[2 * p, o] for o in range(3)]
            lower = [band[2 * p + 1, o] for o in range(3)]
            weights = jnp.concatenate(
                [
                    jnp.concatenate(upper + [zero], axis=1),
                    jnp.concatenate([zero] + lower, axis=1),
                ],
                axis=0,
            )
            total = jnp.dot(
                weights,
                as_rows(cur[it][pl.ds(p * (2 * tile // GROUP), 4 * tile // GROUP)]),
                preferred_element_type=jnp.float32,
            )
            acc[pl.ds(p * (2 * tile // SUB), 2 * tile // SUB)] = total.reshape(
                2 * tile // SUB, SUB, classes
            )

    inner = pairs - 2
    unroll = max(u for u in range(1, BAND_UNROLL + 1) if inner % u == 0)

    def band_inside(it):
        @pl.loop(0, inner // unroll)
        def _(q):
            band_pairs(it, q * unroll + 1, unroll)

    def band_edges(it):
        band_pairs(it, 0, 1)
        band_pairs(it, pairs - 1, 1)

    def far_dot(it, c, start, size):
        return jnp.dot(
            placed[pl.ds(pl.multiple_of(start, size), size), :],
            recv[it, c].reshape(far_rows, width),
            preferred_element_type=jnp.float32,
        )

    def far_add(it, c):
        size = 2 * tile

        @pl.loop(0, pairs // FAR_UNROLL)
        def _(q):
            for u in range(FAR_UNROLL):
                p = q * FAR_UNROLL + u
                here = pl.ds(p * (size // SUB), size // SUB)
                acc[here, :, columns(c)] += far_dot(it, c, p * size, size).reshape(
                    size // SUB, SUB, width
                )

    def far_pass(it, p, into):
        into[...] = far_dot(it, CHUNKS - 1, p * (2 * tile), 2 * tile)

    def finish(it, p, far):
        last = it == ITERS - 1
        target = out_ref if last else cur[1 - it]
        for half in range(2):
            total = jnp.zeros((8, LANE), jnp.float32)
            for r in range(0, tile, ROWS):
                row = p * (2 * tile) + half * tile + r
                here8 = pl.ds(row // SUB, ROWS // SUB)
                here16 = pl.ds(row // GROUP, ROWS // GROUP)
                padded = pl.ds(row // GROUP + tile // GROUP, ROWS // GROUP)
                local = slice(half * tile + r, half * tile + r + ROWS)
                spread = []
                for c in range(0, classes, WIDE):
                    value = acc[here8, :, c : c + WIDE].reshape(ROWS, WIDE)
                    start = (CHUNKS - 1) * width
                    if c >= start:
                        value = value + far[local, c - start : c - start + WIDE]
                    spread.append(value)
                squares = spread[0] * spread[0]
                for s in spread[1:]:
                    squares = squares + s * s
                mean = jnp.sum(squares, axis=1, keepdims=True) * (1.0 / classes)
                signed = limit[here8].reshape(ROWS, LANE)
                factor = jnp.minimum(lax.rsqrt(mean), jnp.abs(signed))
                if not last:
                    fac[here8] = jnp.where(signed < 0.0, 1.0, factor).reshape(
                        ROWS // SUB, SUB, LANE
                    )
                factor = jnp.concatenate([factor] * (WIDE // LANE), axis=1)
                keep = kept[here16] > 0.5
                written = here16 if last else padded
                moved = None
                for q, s in enumerate(spread):
                    where = slice(q * WIDE, (q + 1) * WIDE)
                    before = cur[it][padded, :, where]
                    scaled = (s * factor).reshape(ROWS // GROUP, GROUP, WIDE)
                    fresh = jnp.where(keep, before, scaled.astype(jnp.bfloat16))
                    target[written, :, where] = fresh
                    change = jnp.abs(fresh - before)
                    moved = change if moved is None else moved + change
                moved = moved.astype(jnp.float32).reshape(ROWS, WIDE)
                for i in range(0, ROWS, 8):
                    for c in range(0, WIDE, LANE):
                        total = total + moved[i : i + 8, c : c + LANE]
            part[2 * p + half] = total

    def prepare():
        wide_t[...] = farw[...].astype(jnp.float32).T
        tile_of = lax.broadcasted_iota(jnp.int32, (tiles, n), 0)
        block_of = lax.shift_right_logical(
            lax.broadcasted_iota(jnp.int32, (n, far_rows), 1), blk.bit_length() - 1
        )
        peer_of = lax.broadcasted_iota(jnp.int32, (n, far_rows), 0)
        table = jnp.zeros((tiles, far_rows), jnp.float32)
        for k in range(slots):
            target = jnp.where(count_ref[...] > k, tile_ref[k : k + 1, :], -1)
            chosen = (tile_of == target).astype(jnp.float32)
            spread = (block_of == peer_of * slots + k).astype(jnp.float32)
            table = table + jnp.dot(
                chosen.astype(jnp.bfloat16),
                spread.astype(jnp.bfloat16),
                preferred_element_type=jnp.float32,
            )
        onehot[...] = table

        @pl.loop(0, tiles // PREP_UNROLL)
        def _(q):
            for u in range(PREP_UNROLL):
                t = q * PREP_UNROLL + u
                base = pl.multiple_of(t * tile, tile)
                weights = wide_t[...] * onehot[pl.ds(t, 1), :]
                placed[pl.ds(base, tile), :] = weights.astype(jnp.bfloat16)
                total = band[t, 0].astype(jnp.float32)
                for o in range(1, 3):
                    total = total + band[t, o].astype(jnp.float32)
                for c in range(0, far_rows, LANE):
                    total = total + weights[:, c : c + LANE]
                degree = jnp.sum(total, axis=1, keepdims=True)
                seeded = jnp.broadcast_to(seed_ref[pl.ds(t, 1), :].astype(jnp.float32), (tile, tile)).T
                bound = jnp.broadcast_to(1.0 / (FLOOR * degree), (tile, tile))
                signed = jnp.where(seeded == 1.0, -bound, bound)
                limit[pl.ds(t * (tile // SUB), tile // SUB)] = signed.reshape(tile // SUB, SUB, tile)
                seeded = jnp.concatenate([seeded] * (WIDE // LANE), axis=1).astype(jnp.bfloat16)
                kept[pl.ds(t * (tile // GROUP), tile // GROUP)] = seeded.reshape(
                    tile // GROUP, GROUP, WIDE
                )

    copies = halo_first
    farw_copy.wait()
    band_copy.wait()
    prepare()
    lab_copy.wait()
    own_req.wait()
    pltpu.make_async_copy(req_s.at[others], req_s.at[others], req_recv).wait()
    exchange(0, 0)
    for it in range(ITERS):
        last = it == ITERS - 1
        band_inside(it)
        if it == 0:
            for c in range(1, CHUNKS):
                exchange(0, c)
            await_halo(it, copies)
            band_edges(it)
        for c in range(CHUNKS - 1):
            if it > 0:
                if c == 0:
                    await_factors()
                await_blocks(it, c)
                scale_received(it, c)
                if c == 0:
                    await_halo(it, copies)
                    band_edges(it)
            else:
                await_blocks(it, c)
            far_add(it, c)
            if not last:
                exchange(it + 1, c, raw=True)
        await_blocks(it, CHUNKS - 1)

        if not last:
            copies = halo_copies(
                it + 1, cur[it + 1].at[groups(tile, tile)], cur[it + 1].at[groups(rows, tile)]
            )

        def pair_at(i):
            return lax.rem(i + pairs - 1, pairs)

        far_pass(it, pair_at(0), far_a)

        @pl.loop(0, pairs // 2)
        def _(q):
            far_pass(it, pair_at(2 * q + 1), far_b)
            finish(it, pair_at(2 * q), far_a)
            far_pass(it, pair_at(2 * q + 2), far_a)
            finish(it, pair_at(2 * q + 1), far_b)
            if not last:

                @pl.when(q == 1)
                def _():
                    for copy in copies:
                        copy.start()

        if not last:
            exchange_factors()
            exchange(it + 1, CHUNKS - 1)

        sums = jnp.sum(part[...], axis=1)
        res_ref[it : it + 1, :] = jnp.sum(sums.T, axis=0, keepdims=True)

    sent = req_s.at[others]
    pltpu.make_async_copy(sent, sent, req_send).wait()


def body(labels, seed_mask, band_w, far_block, far_tile, far_count, far_w):
    rows, classes = labels.shape
    tiles, _, tile, _ = band_w.shape
    _, n, slots, blk, _ = far_w.shape
    per = slots * blk
    width = classes // CHUNKS
    dims = (n, tiles, tile, slots, blk, classes)
    vmem, anywhere = pltpu.VMEM, pl.BlockSpec(memory_space=pl.ANY)
    held = pl.BlockSpec(memory_space=pltpu.VMEM)
    dma = pltpu.SemaphoreType.DMA
    bf16, f32 = jnp.bfloat16, jnp.float32
    out, residual = pl.pallas_call(
        functools.partial(kernel, dims),
        out_shape=(
            pltpu.VMEM((rows // GROUP, GROUP, classes), bf16),
            jax.ShapeDtypeStruct((ITERS, tiles), f32),
        ),
        in_specs=[anywhere, anywhere, anywhere, held, held, held, held],
        out_specs=(held, held),
        scratch_shapes=[
            vmem(((rows + 2 * tile) // GROUP, GROUP, classes), bf16),
            vmem(((rows + 2 * tile) // GROUP, GROUP, classes), bf16),
            vmem(band_w.shape, bf16),
            vmem((n * per, tile), bf16),
            vmem((tile, n * per), f32),
            vmem((tiles, n * per), f32),
            vmem((rows, n * per), bf16),
            vmem((rows // SUB, SUB, classes), f32),
            vmem((2 * tile, width), f32),
            vmem((2 * tile, width), f32),
            vmem((rows // SUB, SUB, LANE), f32),
            vmem((rows // GROUP, GROUP, WIDE), bf16),
            vmem((rows // SUB, SUB, LANE), f32),
            vmem((tiles, 8, LANE), f32),
            vmem((2, tile // GROUP, GROUP, classes), bf16),
            vmem((2, tile // GROUP, GROUP, classes), bf16),
            vmem((ITERS, CHUNKS, n, per, width), bf16),
            vmem((ITERS, CHUNKS, n, per, width), bf16),
            vmem((n, 1, LANE), f32),
            vmem((n, 1, LANE), f32),
            pltpu.SMEM((n, slots, n), jnp.int32),
            dma, dma, dma, dma,
            dma, dma,
            dma((ITERS, 2)), dma((ITERS, 2)),
            dma((ITERS, CHUNKS)), dma((ITERS, CHUNKS)),
            dma, dma,
        ],
        compiler_params=pltpu.CompilerParams(
            collective_id=0, has_side_effects=True, vmem_limit_bytes=56 * 1024 * 1024
        ),
    )(
        labels.reshape(rows // GROUP, GROUP, classes),
        band_w,
        far_w.reshape(n * per, tile),
        far_block[0].T,
        far_tile[0].T,
        far_count,
        seed_mask.reshape(tiles, tile),
    )
    return out.reshape(rows, classes), residual


def solution(mesh):
    placed = (
        P("node", None),
        P("node"),
        P("node", None, None, None),
        P("node", None, None),
        P("node", None, None),
        P("node", None),
        P("node", None, None, None, None),
    )
    return jax.shard_map(
        body,
        mesh=mesh,
        in_specs=placed,
        out_specs=(P("node", None), P(None, "node")),
        check_vma=False,
    )
```

```python
import functools

import jax
import jax.numpy as jnp
from jax import lax
from jax.experimental import pallas as pl
from jax.experimental.pallas import tpu as pltpu
from jax.sharding import PartitionSpec as P

ITERS = 2
CHUNKS = 2
MESH = pl.DeviceIdType.MESH
ROWS = 32
GROUP = 16
SUB = 8
LANE = 128
WIDE = 256
FLOOR = 0.05
BAND_UNROLL = 7
NORM_UNROLL = 4
SEND_UNROLL = 4
SCALE_UNROLL = 16
CLOSE_UNROLL = 4
PEER_UNROLL = 6
PREP_UNROLL = 4
VMEM_BYTES = 62 * 1024 * 1024


def finish_pair(p, pieces, acc, far, limit, fac, kept, old, old_at, new, new_at, part):
    classes = acc.shape[2]
    tile = pieces * ROWS // 2
    for half in range(2):
        total = jnp.zeros((8, LANE), jnp.float32)
        for r in range(0, tile, ROWS):
            row = half * tile + r
            at8 = p * (2 * tile // SUB) + row // SUB
            at16 = p * (2 * tile // GROUP) + row // GROUP
            here8 = pl.ds(at8, ROWS // SUB)
            here16 = pl.ds(at16, ROWS // GROUP)
            before_at = pl.ds(at16 + old_at, ROWS // GROUP)
            written = pl.ds(at16 + new_at, ROWS // GROUP)
            local = slice(half * tile + r, half * tile + r + ROWS)
            spread = []
            for c in range(0, classes, WIDE):
                value = acc[here8, :, c : c + WIDE].reshape(ROWS, WIDE)
                if far is not None:
                    start = classes - far.shape[1]
                    if c >= start:
                        value = value + far[local, c - start : c - start + WIDE]
                spread.append(value)
            if far is not None:
                squares = spread[0] * spread[0]
                for s in spread[1:]:
                    squares = squares + s * s
                mean = jnp.sum(squares, axis=1, keepdims=True) * (1.0 / classes)
                signed = limit[here8].reshape(ROWS, LANE)
                factor = jnp.minimum(lax.rsqrt(mean), jnp.abs(signed))
            else:
                factor = fac[here8].reshape(ROWS, LANE)
            factor = jnp.concatenate([factor] * (WIDE // LANE), axis=1)
            keep = kept[here16] > 0.5
            moved = None
            for q, s in enumerate(spread):
                where = slice(q * WIDE, (q + 1) * WIDE)
                before = old[before_at, :, where]
                scaled = (s * factor).reshape(ROWS // GROUP, GROUP, WIDE)
                fresh = jnp.where(keep, before, scaled.astype(jnp.bfloat16))
                new[written, :, where] = fresh
                change = jnp.abs(fresh - before)
                moved = change if moved is None else moved + change
            moved = moved.astype(jnp.float32).reshape(ROWS, WIDE)
            for i in range(0, ROWS, 8):
                for c in range(0, WIDE, LANE):
                    total = total + moved[i : i + 8, c : c + LANE]
        part[2 * p + half] = total


def tile_sums(part):
    sums = jnp.sum(part[...], axis=1)
    return jnp.sum(sums.T, axis=0, keepdims=True)


def closing(
    dims,
    acc, placed, coming, cur1, limit, kept, first_ref,
    out_ref, res_ref,
    far_a, far_b, staged, part, out_sem,
):
    tiles, tile = dims
    pairs = tiles // 2
    size = 2 * tile
    far_rows, width = coming.shape[0] * coming.shape[1], coming.shape[2]

    def far_pass(p, into):
        into[...] = jnp.dot(
            placed[pl.ds(pl.multiple_of(p * size, size), size), :],
            coming[...].reshape(far_rows, width),
            preferred_element_type=jnp.float32,
        )

    def finish(p, far):
        finish_pair(
            p, size // ROWS, acc, far, limit, None, kept, cur1, tile // GROUP, staged, 0, part
        )

    def out_copy(p):
        here = pl.ds(p * (size // GROUP), size // GROUP)
        return pltpu.make_async_copy(staged.at[here], out_ref.at[here], out_sem)

    far_pass(0, far_a)
    step = CLOSE_UNROLL if pairs % CLOSE_UNROLL == 0 else 2

    @pl.loop(0, pairs // step)
    def _(q):
        for u in range(0, step, 2):
            p = q * step + u
            far_pass(p + 1, far_b)
            finish(p, far_a)
            after = p + 2
            far_pass(after if u + 2 < step else jnp.where(after >= pairs, 0, after), far_a)
            finish(p + 1, far_b)

        @pl.when(q > 0)
        def _():
            out_copy(q * step - 1).start()

        for u in range(step - 1):
            out_copy(q * step + u).start()

    res_ref[0:1, :] = first_ref[...]
    res_ref[1:2, :] = tile_sums(part)
    out_copy(pairs - 1).start()
    pltpu.make_async_copy(staged, out_ref, out_sem).wait()


def kernel(
    dims,
    labels_hbm, band_hbm, farw_hbm, req_ref, tile_ref, count_ref, seed_ref,
    acc, placed, coming, cur1, limit, kept, res_ref,
    cur0, band, farw, wide_t, onehot, fac, part,
    halo0, halo1, send, recv0, recv1, fac_out, fac_in, req_s,
    lab_sem, band_sem, farw_sem, smem_sem,
    req_send, req_recv, halo_send, halo_recv, blk_send, blk_recv, fac_send, fac_recv,
):
    n, tiles, tile, slots, blk, classes = dims
    rows = tiles * tile
    per = slots * blk
    far_rows = n * per
    width = classes // CHUNKS
    me = lax.axis_index("node")

    def around(index):
        return jnp.where(index >= n, index - n, index)

    right, left = around(me + 1), around(me + n - 1)
    cur = (cur0, cur1)
    halo = (halo0, halo1)
    landing = {(0, c): recv0.at[c] for c in range(CHUNKS)}
    landing.update({(1, c): recv1.at[c] for c in range(CHUNKS - 1)})
    landing[1, CHUNKS - 1] = coming
    others = pl.ds(0, n - 1)
    pairs = tiles // 2

    def columns(c):
        return slice(c * width, (c + 1) * width)

    def groups(start, size):
        return pl.ds(start // GROUP, size // GROUP)

    def as_rows(value):
        return value.reshape(-1, value.shape[-1])

    barrier = pltpu.get_barrier_semaphore()

    def each_peer(act):
        whole = (n - 1) // PEER_UNROLL

        @pl.loop(0, whole)
        def _(q):
            for u in range(PEER_UNROLL):
                act(around(me + q * PEER_UNROLL + u + 1))

        for j in range(whole * PEER_UNROLL + 1, n):
            act(around(me + j))

    def greet(peer):
        pl.semaphore_signal(barrier, inc=1, device_id=(peer,), device_id_type=MESH)

    each_peer(greet)

    lab_copy = pltpu.make_async_copy(labels_hbm, cur0.at[groups(tile, rows)], lab_sem)
    band_copy = pltpu.make_async_copy(band_hbm, band, band_sem)
    farw_copy = pltpu.make_async_copy(farw_hbm, farw, farw_sem)
    own_req = pltpu.make_async_copy(req_ref, req_s.at[me], smem_sem)
    own_req.start()
    farw_copy.start()
    band_copy.start()
    lab_copy.start()

    pl.semaphore_wait(barrier, n - 1)

    def ask(peer):
        pltpu.make_async_remote_copy(
            req_ref, req_s.at[me], req_send, req_recv,
            device_id=(peer,), device_id_type=MESH,
        ).start()

    each_peer(ask)

    def halo_copies(it, low, high):
        return (
            pltpu.make_async_remote_copy(
                high, halo[it].at[0], halo_send.at[it, 0], halo_recv.at[it, 0],
                device_id=(right,), device_id_type=MESH,
            ),
            pltpu.make_async_remote_copy(
                low, halo[it].at[1], halo_send.at[it, 1], halo_recv.at[it, 1],
                device_id=(left,), device_id_type=MESH,
            ),
        )

    halo_first = halo_copies(
        0, labels_hbm.at[groups(0, tile)], labels_hbm.at[groups(rows - tile, tile)]
    )
    for copy in halo_first:
        copy.start()

    def block_copy(it, c, j):
        peer = around(me + j)
        return pltpu.make_async_remote_copy(
            send.at[it, c, peer], landing[it, c].at[me], blk_send.at[it, c], blk_recv.at[it, c],
            device_id=(peer,), device_id_type=MESH,
        )

    def factor_copy(j):
        peer = around(me + j)
        return pltpu.make_async_remote_copy(
            fac_out.at[peer], fac_in.at[me], fac_send, fac_recv,
            device_id=(peer,), device_id_type=MESH,
        )

    def block_of(it, c, wanted):
        place = lax.shift_right_logical(wanted, 1) + tile // GROUP
        pair = cur[it][place, :, columns(c)].astype(jnp.float32)
        odd = jnp.full((blk, width), lax.bitwise_and(wanted, 1), jnp.int32) == 1
        return jnp.where(odd, pair[blk:], pair[:blk])

    def gathered(it, c, peer, raw):
        halves = []
        for k in range(slots):
            wanted = req_s[peer, k, me]
            if raw:
                seeded = jnp.concatenate([limit[wanted]] * (width // LANE), axis=1) < 0.0
                halves.append(
                    jnp.where(seeded, block_of(0, c, wanted), acc[wanted, :, columns(c)])
                )
            else:
                halves.append(block_of(it, c, wanted))
        return jnp.concatenate(halves, axis=0).astype(jnp.bfloat16)

    def send_all(fill, copy):
        @pl.loop(0, n // SEND_UNROLL)
        def _(q):
            for u in range(SEND_UNROLL):
                fill(around(me + q * SEND_UNROLL + u + 1))

            @pl.when(q > 0)
            def _():
                for u in range(SEND_UNROLL):
                    copy((q - 1) * SEND_UNROLL + u + 1).start()

    def send_rest(copy):
        for j in range(n - SEND_UNROLL + 1, n):
            copy(j).start()

    def exchange(it, c, raw=False):
        def fill(peer):
            send[it, c, peer] = gathered(it, c, peer, raw)

        def copy(j):
            return block_copy(it, c, j)

        send_all(fill, copy)
        landing[it, c][me] = send[it, c, me]
        send_rest(copy)

    diagonal = lax.broadcasted_iota(jnp.int32, (per, LANE), 0) == lax.broadcasted_iota(
        jnp.int32, (per, LANE), 1
    )

    def factors_for(peer):
        both = jnp.concatenate([fac[req_s[peer, k, me]] for k in range(slots)], axis=0)
        return jnp.sum(jnp.where(diagonal, both, 0.0), axis=0, keepdims=True)

    def exchange_factors():
        def fill(peer):
            fac_out[peer] = factors_for(peer)

        send_all(fill, factor_copy)
        fac_in[me] = fac_out[me]
        send_rest(factor_copy)

    def await_factors():
        pltpu.make_async_copy(fac_out.at[others], fac_out.at[others], fac_send).wait()
        pltpu.make_async_copy(fac_in.at[others], fac_in.at[others], fac_recv).wait()

    def await_halo(it, copies):
        for copy in copies:
            copy.wait()
        cur[it][groups(0, tile)] = halo[it][0]
        cur[it][groups(rows + tile, tile)] = halo[it][1]

    def await_blocks(it, c):
        gone, came = send.at[it, c, others], landing[it, c].at[others]
        pltpu.make_async_copy(gone, gone, blk_send.at[it, c]).wait()
        pltpu.make_async_copy(came, came, blk_recv.at[it, c]).wait()

    def scale_received(it, c):
        @pl.loop(0, n // SCALE_UNROLL)
        def _(q):
            for u in range(SCALE_UNROLL):
                s = q * SCALE_UNROLL + u
                column = jnp.sum(
                    jnp.where(diagonal, jnp.broadcast_to(fac_in[s], (per, LANE)), 0.0),
                    axis=1, keepdims=True,
                )
                value = landing[it, c][s].astype(jnp.float32) * column
                landing[it, c][s] = value.astype(jnp.bfloat16)

    def band_pairs(it, first, count):
        zero = jnp.zeros((tile, tile), jnp.bfloat16)
        for u in range(count):
            p = first + u
            upper = [band[2 * p, o] for o in range(3)]
            lower = [band[2 * p + 1, o] for o in range(3)]
            weights = jnp.concatenate(
                [
                    jnp.concatenate(upper + [zero], axis=1),
                    jnp.concatenate([zero] + lower, axis=1),
                ],
                axis=0,
            )
            total = jnp.dot(
                weights,
                as_rows(cur[it][pl.ds(p * (2 * tile // GROUP), 4 * tile // GROUP)]),
                preferred_element_type=jnp.float32,
            )
            acc[pl.ds(p * (2 * tile // SUB), 2 * tile // SUB)] = total.reshape(
                2 * tile // SUB, SUB, classes
            )

    inner = pairs - 2
    unroll = max(u for u in range(1, BAND_UNROLL + 1) if inner % u == 0)

    def band_inside(it):
        @pl.loop(0, inner // unroll)
        def _(q):
            band_pairs(it, q * unroll + 1, unroll)

    def band_edges(it):
        band_pairs(it, 0, 1)
        band_pairs(it, pairs - 1, 1)

    def far_dot(it, c, start, size):
        return jnp.dot(
            placed[pl.ds(pl.multiple_of(start, size), size), :],
            landing[it, c][...].reshape(far_rows, width),
            preferred_element_type=jnp.float32,
        )

    def far_pairs(it, c, first, count):
        size = 2 * tile
        for u in range(count):
            p = first + u
            here = pl.ds(p * (size // SUB), size // SUB)
            acc[here, :, columns(c)] += far_dot(it, c, p * size, size).reshape(
                size // SUB, SUB, width
            )

    def far_inside(it, c):
        @pl.loop(0, inner // unroll)
        def _(q):
            far_pairs(it, c, q * unroll + 1, unroll)

    def far_edges(it, c):
        far_pairs(it, c, 0, 1)
        far_pairs(it, c, pairs - 1, 1)

    def norm_pairs(it, first, count):
        size = 2 * tile
        c = CHUNKS - 1
        for u in range(count):
            p = first + u
            here = pl.ds(p * (size // SUB), size // SUB)
            value = far_dot(it, c, p * size, size)
            value = value + acc[here, :, columns(c)].reshape(size, width)
            acc[here, :, columns(c)] = value.reshape(size // SUB, SUB, width)
            squares = value * value
            for other in range(CHUNKS - 1):
                value = acc[here, :, columns(other)].reshape(size, width)
                squares = squares + value * value
            mean = jnp.sum(squares, axis=1, keepdims=True) * (1.0 / classes)
            signed = limit[here].reshape(size, LANE)
            factor = jnp.minimum(lax.rsqrt(mean), jnp.abs(signed))
            fac[here] = jnp.where(signed < 0.0, 1.0, factor).reshape(size // SUB, SUB, LANE)

    def norm_inside(it):
        @pl.loop(0, inner // unroll)
        def _(q):
            norm_pairs(it, q * unroll + 1, unroll)

    def norm_edges(it):
        norm_pairs(it, 0, 1)
        norm_pairs(it, pairs - 1, 1)

    def finish(p):
        finish_pair(
            p, 2 * tile // ROWS, acc, None, limit, fac, kept, cur0, tile // GROUP,
            cur1, tile // GROUP, part,
        )

    def prepare():
        wide_t[...] = farw[...].astype(jnp.float32).T
        tile_of = lax.broadcasted_iota(jnp.int32, (tiles, n), 0)
        block_of = lax.shift_right_logical(
            lax.broadcasted_iota(jnp.int32, (n, far_rows), 1), blk.bit_length() - 1
        )
        peer_of = lax.broadcasted_iota(jnp.int32, (n, far_rows), 0)
        table = jnp.zeros((tiles, far_rows), jnp.float32)
        for k in range(slots):
            target = jnp.where(count_ref[...] > k, tile_ref[k : k + 1, :], -1)
            chosen = (tile_of == target).astype(jnp.float32)
            spread = (block_of == peer_of * slots + k).astype(jnp.float32)
            table = table + jnp.dot(
                chosen.astype(jnp.bfloat16),
                spread.astype(jnp.bfloat16),
                preferred_element_type=jnp.float32,
            )
        onehot[...] = table

        @pl.loop(0, tiles // PREP_UNROLL)
        def _(q):
            for u in range(PREP_UNROLL):
                t = q * PREP_UNROLL + u
                base = pl.multiple_of(t * tile, tile)
                weights = wide_t[...] * onehot[pl.ds(t, 1), :]
                placed[pl.ds(base, tile), :] = weights.astype(jnp.bfloat16)
                total = band[t, 0].astype(jnp.float32)
                for o in range(1, 3):
                    total = total + band[t, o].astype(jnp.float32)
                for c in range(0, far_rows, LANE):
                    total = total + weights[:, c : c + LANE]
                degree = jnp.sum(total, axis=1, keepdims=True)
                seeded = jnp.broadcast_to(seed_ref[pl.ds(t, 1), :].astype(jnp.float32), (tile, tile)).T
                bound = jnp.broadcast_to(1.0 / (FLOOR * degree), (tile, tile))
                signed = jnp.where(seeded == 1.0, -bound, bound)
                limit[pl.ds(t * (tile // SUB), tile // SUB)] = signed.reshape(tile // SUB, SUB, tile)
                seeded = jnp.concatenate([seeded] * (WIDE // LANE), axis=1).astype(jnp.bfloat16)
                kept[pl.ds(t * (tile // GROUP), tile // GROUP)] = seeded.reshape(
                    tile // GROUP, GROUP, WIDE
                )

    copies = halo_first
    farw_copy.wait()
    band_copy.wait()
    prepare()
    lab_copy.wait()
    own_req.wait()
    pltpu.make_async_copy(req_s.at[others], req_s.at[others], req_recv).wait()
    exchange(0, 0)
    final = CHUNKS - 1

    band_inside(0)
    for c in range(1, CHUNKS):
        exchange(0, c)
    await_halo(0, copies)
    band_edges(0)
    for c in range(final):
        await_blocks(0, c)
        far_inside(0, c)
        far_edges(0, c)
        exchange(1, c, raw=True)
    await_blocks(0, final)
    norm_edges(0)
    finish(0)
    finish(pairs - 1)
    copies = halo_copies(1, cur[1].at[groups(tile, tile)], cur[1].at[groups(rows, tile)])
    norm_inside(0)
    exchange_factors()
    for copy in copies:
        copy.start()
    exchange(1, final, raw=True)

    @pl.loop(1, pairs - 1)
    def _(p):
        finish(p)

    res_ref[...] = tile_sums(part)
    band_inside(1)
    await_factors()
    for c in range(final):
        await_blocks(1, c)
        scale_received(1, c)
        far_inside(1, c)
    await_halo(1, copies)
    band_edges(1)
    for c in range(final):
        far_edges(1, c)
    await_blocks(1, final)
    scale_received(1, final)
    sent = req_s.at[others]
    pltpu.make_async_copy(sent, sent, req_send).wait()


def body(labels, seed_mask, band_w, far_block, far_tile, far_count, far_w):
    rows, classes = labels.shape
    tiles, _, tile, _ = band_w.shape
    _, n, slots, blk, _ = far_w.shape
    per = slots * blk
    width = classes // CHUNKS
    dims = (n, tiles, tile, slots, blk, classes)
    vmem, anywhere = pltpu.VMEM, pl.BlockSpec(memory_space=pl.ANY)
    held = pl.BlockSpec(memory_space=pltpu.VMEM)
    dma = pltpu.SemaphoreType.DMA
    bf16, f32 = jnp.bfloat16, jnp.float32
    passed_on = 4 * rows * (classes + LANE)
    passed_on += 2 * (rows * (n * per + WIDE) + n * per * width + (rows + 2 * tile) * classes)
    *kept_in_vmem, first = pl.pallas_call(
        functools.partial(kernel, dims),
        out_shape=(
            vmem((rows // SUB, SUB, classes), f32),
            vmem((rows, n * per), bf16),
            vmem((n, per, width), bf16),
            vmem(((rows + 2 * tile) // GROUP, GROUP, classes), bf16),
            vmem((rows // SUB, SUB, LANE), f32),
            vmem((rows // GROUP, GROUP, WIDE), bf16),
            vmem((1, tiles), f32),
        ),
        in_specs=[anywhere, anywhere, anywhere, held, held, held, held],
        out_specs=(held,) * 7,
        scratch_shapes=[
            vmem(((rows + 2 * tile) // GROUP, GROUP, classes), bf16),
            vmem(band_w.shape, bf16),
            vmem((n * per, tile), bf16),
            vmem((tile, n * per), f32),
            vmem((tiles, n * per), f32),
            vmem((rows // SUB, SUB, LANE), f32),
            vmem((tiles, 8, LANE), f32),
            vmem((2, tile // GROUP, GROUP, classes), bf16),
            vmem((2, tile // GROUP, GROUP, classes), bf16),
            vmem((ITERS, CHUNKS, n, per, width), bf16),
            vmem((CHUNKS, n, per, width), bf16),
            vmem((CHUNKS - 1, n, per, width), bf16),
            vmem((n, 1, LANE), f32),
            vmem((n, 1, LANE), f32),
            pltpu.SMEM((n, slots, n), jnp.int32),
            dma, dma, dma, dma,
            dma, dma,
            dma((ITERS, 2)), dma((ITERS, 2)),
            dma((ITERS, CHUNKS)), dma((ITERS, CHUNKS)),
            dma, dma,
        ],
        compiler_params=pltpu.CompilerParams(
            collective_id=0, has_side_effects=True,
            vmem_limit_bytes=VMEM_BYTES - passed_on,
        ),
    )(
        labels.reshape(rows // GROUP, GROUP, classes),
        band_w,
        far_w.reshape(n * per, tile),
        far_block[0].T,
        far_tile[0].T,
        far_count,
        seed_mask.reshape(tiles, tile),
    )
    out, residual = pl.pallas_call(
        functools.partial(closing, (tiles, tile)),
        out_shape=(
            jax.ShapeDtypeStruct((rows // GROUP, GROUP, classes), bf16),
            jax.ShapeDtypeStruct((ITERS, tiles), f32),
        ),
        in_specs=[held] * 7,
        out_specs=(anywhere, held),
        scratch_shapes=[
            vmem((2 * tile, width), f32),
            vmem((2 * tile, width), f32),
            vmem((rows // GROUP, GROUP, classes), bf16),
            vmem((tiles, 8, LANE), f32),
            dma,
        ],
        compiler_params=pltpu.CompilerParams(vmem_limit_bytes=12 * 1024 * 1024),
    )(*kept_in_vmem, first)
    return out.reshape(rows, classes), residual


def solution(mesh):
    placed = (
        P("node", None),
        P("node"),
        P("node", None, None, None),
        P("node", None, None),
        P("node", None, None),
        P("node", None),
        P("node", None, None, None, None),
    )
    return jax.shard_map(
        body,
        mesh=mesh,
        in_specs=placed,
        out_specs=(P("node", None), P(None, "node")),
        check_vma=False,
    )
```
